32 devices in a mesh: seq: 4 (over x, core), mp: 8 (over z, y).
Axes of the slice: x: 2, y: 2, z: 4, core: 2. Of those that a mesh axis runs over, the one named last changes fastest.
Arguments:
- byte_states: bfloat16 [4, 4096, 1024], P('seq', 'mp'), may hold values from -312 to 312
- patch_latents: bfloat16 [4, 1024, 4096], P(None, 'seq', 'mp'), may hold values from -6 to 6
- patch_lengths: int32 [4, 1024], P('seq'), may hold values from 1 to 12, 4096 in all within a row
- w_down: bfloat16 [4096, 1024], replicated, may hold values from -0.09375 to 0.09375
- kv_gain: bfloat16 [1024], replicated, may hold values from 0.25 to 1.75
- w_query: bfloat16 [1024, 1024], replicated, may hold values from -0.375 to 0.375
- w_key: bfloat16 [1024, 1024], replicated, may hold values from -0.1875 to 0.1875
- w_value: bfloat16 [1024, 1024], replicated, may hold values from -0.1875 to 0.1875
- w_out: bfloat16 [1024, 1024], replicated, may hold values from -0.375 to 0.375
- out_gain: bfloat16 [1024], replicated, may hold values from 0.25 to 1.75
Outputs:
- decoded: bfloat16 [4, 4096, 1024], P('seq', 'mp')
The draws below stay inside these ranges and needn't reach their ends.
Inputs may be any that keep to these rules, and one draw needn't show every extreme that they name: patch_lengths[s] lists the lengths of the 1024 patches of sequence s in order; they sum to 4096 and the longest is exactly 12.
All inputs are finite; a program needn't handle non-finite values.
Results may differ from the reference program's by a relative error of at most 0.0076.
Values may be sent and summed in bfloat16 or wider, within the bound.
A program may use at most 128 MiB of HBM per device.

```python
import math
import jax
import jax.numpy as jnp
import numpy as np
from jax import lax

D = 1024
GD = 4096
HEADS = 16
HEAD_DIM = 64
MOST = 12
SEQ_LEN = 4096
PATCHES = 1024
SEQS = 4


def draw_byte_states(key, part):
    base_key = jax.random.fold_in(key, 0)
    values = jnp.clip(jax.random.normal(base_key, (SEQS, SEQ_LEN, D), jnp.float32), -6.0, 6.0)
    return values.astype(jnp.bfloat16)


def steps_of(own_key, dims, cuts, least, largest):
    level, own = 1.0, jax.random.fold_in(own_key, 6)
    for dim, parts in cuts:
        heights = jnp.exp(jax.random.uniform(jax.random.fold_in(own, dim), (parts,), jnp.float32, least / len(cuts), largest / len(cuts)))
        level = level * jnp.repeat(heights, dims[dim] // parts).reshape([-1 if axis == dim else 1 for axis in range(len(dims))])
    return level


def length_profile(amount, total, reach, skew):
    loads = [(1 << 20) // math.isqrt(standing ** skew) + 1 for standing in range(2, amount + 1)]
    rest, holding = total - reach - (amount - 1), [1] * (amount - 1)
    while rest > 0:
        free = [i for i in range(amount - 1) if holding[i] < reach]
        pool, left = sum([loads[i] for i in free]), rest
        for i in free:
            extra = min(reach - holding[i], max(1, left * loads[i] // pool), rest)
            holding[i] = holding[i] + extra
            rest = rest - extra
    return np.array([reach] + holding)


def ragged_sizes(stream_key, amount, total, bound, skew):
    if amount == 2:
        one = jax.random.randint(stream_key, (), max(1, total - bound), min(bound, total - 1) + 1)
        return jnp.stack([one, total - one])
    sizes = jnp.asarray(length_profile(amount, total, bound, skew), jnp.int32)
    twos = (amount - 1) // 2
    donor, taker = sizes[1:1 + 2 * twos:2], sizes[2:2 + 2 * twos:2]
    room = jnp.minimum(donor - 1, bound - taker)
    passed = jax.random.randint(jax.random.fold_in(stream_key, 1), (twos,), 0, 1 << 20) % (room + 1)
    sizes = sizes.at[1:1 + 2 * twos:2].set(donor - passed).at[2:2 + 2 * twos:2].set(taker + passed)
    return sizes[jax.random.permutation(jax.random.fold_in(stream_key, 2), amount)]


def centred(rng, shape, width, reach, shards=(), kind=jnp.bfloat16):
    entries = width * jax.random.normal(rng, shape, jnp.float32)
    if shards:
        entries = entries * steps_of(rng, shape, shards, -0.22, 0.18)
    return jnp.clip(entries, -reach, reach).astype(kind)


def setup_inputs(seed: int = 0) -> dict:
    seeds = jax.random.split(jax.random.key(seed), 11)
    return {
        "byte_states": draw_byte_states(jax.random.fold_in(seeds[10], 71), 0),
        "patch_latents": centred(seeds[1], (SEQS, PATCHES, GD), 1.0, 6.0, ((1, 4), (2, 8))),
        "patch_lengths": jax.vmap(lambda own: ragged_sizes(own, PATCHES, SEQ_LEN, MOST, 2))(jax.random.split(seeds[2], SEQS)).reshape((SEQS, PATCHES)).astype(jnp.int32),
        "w_down": centred(seeds[3], (GD, D), GD ** -0.5, 0.09375),
        "kv_gain": jnp.clip(1.0 + 0.15 * jax.random.normal(seeds[4], (D,), jnp.float32), 0.25, 1.75).astype(jnp.bfloat16),
        "w_query": centred(seeds[5], (D, D), (D // 4) ** -0.5, 0.375),
        "w_key": centred(seeds[6], (D, D), D ** -0.5, 0.1875),
        "w_value": centred(seeds[7], (D, D), D ** -0.5, 0.1875),
        "w_out": centred(seeds[8], (D, D), (D // 4) ** -0.5, 0.375),
        "out_gain": jnp.clip(1.0 + 0.15 * jax.random.normal(seeds[9], (D,), jnp.float32), 0.25, 1.75).astype(jnp.bfloat16),
    }


def rms_norm(values, gain_row):
    mean_square = lax.optimization_barrier(jnp.mean(values * values, axis=-1, keepdims=True))
    return values * lax.rsqrt(mean_square + 1e-05) * gain_row.astype(jnp.float32)

def attend(query_block, position_block, key_rows, value_rows, starts):
    row_count = query_block.shape[0]
    scale_factor = 1.0 / math.sqrt(HEAD_DIM)
    query_heads = query_block.astype(jnp.float32).reshape(row_count, HEADS, HEAD_DIM)
    key_heads = key_rows.astype(jnp.float32).reshape(-1, HEADS, HEAD_DIM)
    value_heads = value_rows.astype(jnp.float32).reshape(-1, HEADS, HEAD_DIM)
    scores = jnp.einsum('rhd,khd->hrk', query_heads, key_heads) * scale_factor
    allowed = starts[None, None, :] <= position_block[None, :, None]
    masked = jnp.where(allowed, scores, -1e+30)
    row_max = lax.optimization_barrier(jnp.max(masked, axis=-1, keepdims=True))
    raised = jnp.where(allowed, jnp.exp(masked - row_max), 0.0)
    totals = lax.optimization_barrier(jnp.sum(raised, axis=-1))
    weights = raised.astype(jnp.bfloat16).astype(jnp.float32)
    summed = jnp.einsum('hrk,khd->hrd', weights, value_heads) / totals[..., None]
    return jnp.transpose(summed, (1, 0, 2)).reshape(row_count, D).astype(jnp.bfloat16)

def reference(byte_states, patch_latents, patch_lengths, w_down, kv_gain, w_query, w_key, w_value, w_out, out_gain):
    decoded_rows = []
    block_rows = math.gcd(SEQ_LEN, 512)
    for sequence in range(SEQS):
        projected = jnp.dot(patch_latents[sequence], w_down, preferred_element_type=jnp.float32)
        patch_normed = rms_norm(projected, kv_gain).astype(jnp.bfloat16)
        key_rows = jnp.dot(patch_normed, w_key, preferred_element_type=jnp.float32).astype(jnp.bfloat16)
        value_rows = jnp.dot(patch_normed, w_value, preferred_element_type=jnp.float32).astype(jnp.bfloat16)
        lengths = patch_lengths[sequence].astype(jnp.int32)
        starts = jnp.cumsum(lengths).astype(jnp.int32) - lengths
        queries = jnp.dot(byte_states[sequence], w_query, preferred_element_type=jnp.float32).astype(jnp.bfloat16)
        query_blocks = queries.reshape(SEQ_LEN // block_rows, block_rows, D)
        position_blocks = jnp.arange(SEQ_LEN, dtype=jnp.int32).reshape(SEQ_LEN // block_rows, block_rows)

        def attend_rows(packed):
            return attend(packed[0], packed[1], key_rows, value_rows, starts)
        head_out = lax.map(attend_rows, (query_blocks, position_blocks)).reshape(SEQ_LEN, D)
        residual = byte_states[sequence].astype(jnp.float32) + jnp.dot(head_out, w_out, preferred_element_type=jnp.float32)
        decoded_rows.append(rms_norm(residual, out_gain).astype(jnp.bfloat16))
    return jnp.stack(decoded_rows)
```

```python
import functools

import jax
import jax.numpy as jnp
from jax import lax
from jax.experimental import pallas as pl
from jax.experimental.pallas import tpu as pltpu
from jax.sharding import PartitionSpec as P

HEADS = 16
HEAD_DIM = 64
MASKED = -1e30
MESH = pl.DeviceIdType.MESH


def rms_norm(values, gain_row):
    mean_square = jnp.mean(values * values, axis=-1, keepdims=True)
    return values * lax.rsqrt(mean_square + 1e-05) * gain_row


def exchange_kernel(
    n_seq, n_mp, inner,
    lat, wd, gain, bs, wq, wk, wv,
    q_out, k_out, v_out,
    latbuf, gbuf, acc, wd_v, bs_v, wq_v, wk_v, wv_v,
    load_sem, send_sem, recv_sem, up_sem, down_sem, pair_sem, got_sem,
):
    my_s = lax.axis_index("seq")
    my_m = lax.axis_index("mp")
    total = n_seq * n_mp
    me = my_s * n_mp + my_m
    piece = lat.shape[1] // n_mp
    feats = lat.shape[2]
    width = acc.shape[1]
    tile = 256

    loads = [
        pltpu.make_async_copy(src, dst, load_sem.at[i])
        for i, (src, dst) in enumerate(
            [(bs, bs_v), (wq, wq_v), (wd, wd_v), (wk, wk_v), (wv, wv_v)]
        )
    ]
    for load in loads:
        load.start()

    barrier = pltpu.get_barrier_semaphore()

    def greet(step, carry):
        other = lax.rem(me + step, total)
        pl.semaphore_signal(
            barrier, inc=1,
            device_id={"seq": other // n_mp, "mp": lax.rem(other, n_mp)},
            device_id_type=MESH,
        )
        return carry

    lax.fori_loop(1, total, greet, 0)
    pl.semaphore_wait(barrier, total - 1)

    def piece_copy(other):
        t, m = other // n_mp, lax.rem(other, n_mp)
        return pltpu.make_async_remote_copy(
            src_ref=lat.at[t, pl.ds(pl.multiple_of(m * piece, piece), piece), :],
            dst_ref=latbuf.at[my_m, pl.ds(pl.multiple_of(my_s * piece, piece), piece), :],
            send_sem=send_sem.at[other],
            recv_sem=recv_sem.at[me],
            device_id={"seq": t, "mp": m},
            device_id_type=MESH,
        )

    def piece_arrival(s, m):
        here = latbuf.at[m, pl.ds(pl.multiple_of(s * piece, piece), piece), :]
        return pltpu.make_async_copy(here, here, recv_sem.at[s * n_mp + m])

    def send_piece(step, carry):
        piece_copy(lax.rem(me + step, total)).start()
        return carry

    lax.fori_loop(1, total, send_piece, 0)
    pltpu.make_async_copy(
        lat.at[my_s, pl.ds(pl.multiple_of(my_m * piece, piece), piece), :],
        latbuf.at[my_m, pl.ds(pl.multiple_of(my_s * piece, piece), piece), :],
        recv_sem.at[me],
    ).start()

    loads[0].wait()
    loads[1].wait()

    def query_tile(j, carry):
        cols = pl.ds(pl.multiple_of(j * tile, tile), tile)
        made = jnp.dot(bs_v[...], wq_v[:, cols], preferred_element_type=jnp.float32)
        q_out[:, cols] = made.astype(jnp.bfloat16) * jnp.bfloat16(HEAD_DIM**-0.5)
        return carry

    lax.fori_loop(0, wq_v.shape[1] // tile, query_tile, 0)

    loads[2].wait()
    acc[...] = jnp.zeros_like(acc)

    def project(step, carry):
        m = lax.rem(my_m + step, n_mp)

        def arrived(s, inner_carry):
            piece_arrival(s, m).wait()
            return inner_carry

        lax.fori_loop(0, n_seq, arrived, 0)
        rows = pl.ds(pl.multiple_of(m * feats, feats), feats)
        acc[...] += jnp.dot(latbuf[m], wd_v[rows, :], preferred_element_type=jnp.float32)
        return carry

    lax.fori_loop(0, n_mp, project, 0)
    gbuf[my_m] = rms_norm(acc[...], gain[...].astype(jnp.float32)).astype(jnp.bfloat16)

    outer = n_mp // inner
    my_o = my_m // inner
    my_i = lax.rem(my_m, inner)
    partner = my_o * inner + (inner - 1 - my_i)

    def row_copy(chunk, sem, target):
        return pltpu.make_async_remote_copy(
            src_ref=gbuf.at[chunk],
            dst_ref=gbuf.at[chunk],
            send_sem=sem.at[chunk],
            recv_sem=got_sem.at[chunk],
            device_id={"seq": my_s, "mp": target},
            device_id_type=MESH,
        )

    def wait_chunk(chunk):
        pltpu.make_async_copy(gbuf.at[chunk], gbuf.at[chunk], got_sem.at[chunk]).wait()

    def go_up(chunk):
        return row_copy(chunk, up_sem, my_m + inner)

    def go_down(chunk):
        return row_copy(chunk, down_sem, my_m - inner)

    def go_pair(chunk):
        return row_copy(chunk, pair_sem, partner)

    has_up = my_o < outer - 1
    has_down = my_o > 0
    pl.when(has_up)(lambda: go_up(my_m).start())
    pl.when(has_down)(lambda: go_down(my_m).start())
    go_pair(my_m).start()

    def relay(k, carry):
        below = my_m - k * inner
        above = my_m + k * inner

        @pl.when(my_o - k >= 0)
        def _():
            wait_chunk(below)
            pl.when(has_up)(lambda: go_up(below).start())
            go_pair(below).start()

        @pl.when(my_o + k < outer)
        def _():
            wait_chunk(above)
            pl.when(has_down)(lambda: go_down(above).start())
            go_pair(above).start()

        return carry

    lax.fori_loop(1, outer, relay, 0)

    def take_pair(o, carry):
        wait_chunk(o * inner + (inner - 1 - my_i))
        return carry

    lax.fori_loop(0, outer, take_pair, 0)
    loads[3].wait()
    loads[4].wait()

    def kv_tile(j, carry):
        cols = pl.ds(pl.multiple_of(j * tile, tile), tile)
        for c in range(n_mp // 8):
            normed = gbuf[pl.ds(c * 8, 8)].reshape(8 * gbuf.shape[1], width)
            rows = pl.ds(c * 8 * gbuf.shape[1], 8 * gbuf.shape[1])
            k_out[rows, cols] = jnp.dot(
                normed, wk_v[:, cols], preferred_element_type=jnp.float32
            ).astype(jnp.bfloat16)
            v_out[rows, cols] = jnp.dot(
                normed, wv_v[:, cols], preferred_element_type=jnp.float32
            ).astype(jnp.bfloat16)
        return carry

    lax.fori_loop(0, wk_v.shape[1] // tile, kv_tile, 0)

    def finish_piece(step, carry):
        piece_copy(lax.rem(me + step, total)).wait_send()
        return carry

    lax.fori_loop(1, total, finish_piece, 0)

    def finish_rows(o, carry):
        chunk = o * inner + my_i
        pl.when(has_up & (o <= my_o))(lambda: go_up(chunk).wait_send())
        pl.when(has_down & (o >= my_o))(lambda: go_down(chunk).wait_send())
        go_pair(chunk).wait_send()
        return carry

    lax.fori_loop(0, outer, finish_rows, 0)


def attend_kernel(
    rows, q, k, v, starts, positions, bs, w_out, out_gain, out, bias, v_ext, head_out
):
    pair = pl.program_id(0)
    tokens = bias.shape[0]
    lanes = q.shape[1]

    @pl.when(pair == 0)
    def _():
        bias[...] = jnp.where(starts[...] <= positions[...], 0.0, MASKED)
        v_ext[:, lanes:] = jnp.ones((v_ext.shape[0], lanes), v_ext.dtype)

    v_ext[:, :lanes] = v[...]
    lane = lax.broadcasted_iota(jnp.int32, (rows, lanes), 1)
    low = lane < HEAD_DIM

    def one_block(b, carry):
        at = pl.ds(pl.multiple_of(b * rows, rows), rows)
        both = q[at, :]
        parts = []
        for half in range(2):
            keep = low if half == 0 else ~low
            q_half = jnp.where(keep, both, jnp.zeros_like(both))
            scores = lax.dot_general(
                q_half, k[...], (((1,), (1,)), ((), ())), preferred_element_type=jnp.float32
            ) + bias[at, :]
            weights = jnp.exp(scores - jnp.max(scores, axis=-1, keepdims=True))
            summed = jnp.dot(
                weights.astype(jnp.bfloat16), v_ext[...], preferred_element_type=jnp.float32
            )
            parts.append(summed[:, :lanes] / summed[:, lanes:])
        head_out[pair, at, :] = jnp.where(low, parts[0], parts[1]).astype(jnp.bfloat16)
        return carry

    blocks = tokens // rows
    lax.fori_loop(0, blocks, one_block, 0, unroll=blocks <= 2)

    @pl.when(pair == pl.num_programs(0) - 1)
    def _():
        joined = jnp.concatenate([head_out[p] for p in range(head_out.shape[0])], axis=1)
        residual = bs[...].astype(jnp.float32) + jnp.dot(
            joined, w_out[...], preferred_element_type=jnp.float32
        )
        out[...] = rms_norm(residual, out_gain[...].astype(jnp.float32)).astype(out.dtype)


def per_device(n_seq, n_mp, byte_states, patch_latents, patch_lengths, w_down, kv_gain,
               w_query, w_key, w_value, w_out, out_gain):
    own_rows = byte_states[0]
    tokens, width = own_rows.shape
    patches = patch_lengths.shape[1]
    here = patches // n_mp
    feats = patch_latents.shape[2]
    inner = 2
    any_spec = pl.BlockSpec(memory_space=pl.ANY)
    vmem_spec = pl.BlockSpec(memory_space=pltpu.VMEM)
    bf16 = jnp.bfloat16
    queries, key_rows, value_rows = pl.pallas_call(
        functools.partial(exchange_kernel, n_seq, n_mp, inner),
        name="exchange",
        out_shape=(
            jax.ShapeDtypeStruct((tokens, width), bf16),
            jax.ShapeDtypeStruct((patches, width), bf16),
            jax.ShapeDtypeStruct((patches, width), bf16),
        ),
        in_specs=[any_spec, any_spec, vmem_spec] + [any_spec] * 4,
        out_specs=(vmem_spec,) * 3,
        scratch_shapes=[
            pltpu.VMEM((n_mp, here, feats), bf16),
            pltpu.VMEM((n_mp, here, width), bf16),
            pltpu.VMEM((here, width), jnp.float32),
            pltpu.VMEM(w_down.shape, bf16),
            pltpu.VMEM((tokens, width), bf16),
            pltpu.VMEM(w_query.shape, bf16),
            pltpu.VMEM(w_key.shape, bf16),
            pltpu.VMEM(w_value.shape, bf16),
            pltpu.SemaphoreType.DMA((5,)),
            pltpu.SemaphoreType.DMA((n_seq * n_mp,)),
            pltpu.SemaphoreType.DMA((n_seq * n_mp,)),
            pltpu.SemaphoreType.DMA((n_mp,)),
            pltpu.SemaphoreType.DMA((n_mp,)),
            pltpu.SemaphoreType.DMA((n_mp,)),
            pltpu.SemaphoreType.DMA((n_mp,)),
        ],
        compiler_params=pltpu.CompilerParams(
            collective_id=0, has_side_effects=True, vmem_limit_bytes=60 * 1024 * 1024
        ),
    )(patch_latents, w_down, kv_gain[None], own_rows, w_query, w_key, w_value)

    lengths = patch_lengths[0]
    starts = jnp.cumsum(lengths) - lengths
    starts = starts.reshape(n_seq, n_mp, here // n_seq).transpose(1, 0, 2).reshape(1, patches)
    positions = (
        lax.axis_index("mp") * tokens + lax.broadcasted_iota(jnp.int32, (tokens, 1), 0)
    )
    lanes = 2 * HEAD_DIM
    rows = max(16, min(256, (256 * 1024) // patches))
    whole = lambda shape: pl.BlockSpec(shape, lambda p: (0, 0))
    decoded = pl.pallas_call(
        functools.partial(attend_kernel, rows),
        name="attend",
        grid=(width // lanes,),
        out_shape=jax.ShapeDtypeStruct((tokens, width), bf16),
        in_specs=[
            pl.BlockSpec((tokens, lanes), lambda p: (0, p)),
            pl.BlockSpec((patches, lanes), lambda p: (0, p)),
            pl.BlockSpec((patches, lanes), lambda p: (0, p)),
            whole((1, patches)),
            whole((tokens, 1)),
            whole((tokens, width)),
            whole((width, width)),
            whole((1, width)),
        ],
        out_specs=whole((tokens, width)),
        scratch_shapes=[
            pltpu.VMEM((tokens, patches), jnp.float32),
            pltpu.VMEM((patches, 2 * lanes), bf16),
            pltpu.VMEM((width // lanes, tokens, lanes), bf16),
        ],
        compiler_params=pltpu.CompilerParams(
            dimension_semantics=("arbitrary",), vmem_limit_bytes=60 * 1024 * 1024
        ),
    )(queries, key_rows, value_rows, starts, positions, own_rows, w_out, out_gain[None])
    return decoded[None]


def solution(mesh):
    return jax.shard_map(
        functools.partial(per_device, mesh.shape["seq"], mesh.shape["mp"]),
        mesh=mesh,
        in_specs=(
            P("seq", "mp", None),
            P(None, "seq", "mp"),
            P("seq", None),
            P(), P(), P(), P(), P(), P(), P(),
        ),
        out_specs=P("seq", "mp", None),
        check_vma=False,
    )
```

```python
import functools

import jax
import jax.numpy as jnp
from jax import lax
from jax.experimental import pallas as pl
from jax.experimental.pallas import tpu as pltpu
from jax.sharding import PartitionSpec as P

HEADS = 16
HEAD_DIM = 64
MASKED = -1e30
MESH = pl.DeviceIdType.MESH


def rms_norm(values, gain_row):
    mean_square = jnp.mean(values * values, axis=-1, keepdims=True)
    return values * lax.rsqrt(mean_square + 1e-05) * gain_row


def layer_kernel(
    n_seq, n_mp, inner, parts,
    lat, wd, gain, bs, wq, wk, wv, wo, out_gain, lengths,
    out,
    latbuf, gbuf, acc, wd_v, bs_v, wq_v, wk_v, wv_v, wo_v,
    q_v, k_v, v_v, v_ext, starts_v, bias, num, den, peak, head_out,
    load_sem, send_sem, recv_sem, up_sem, down_sem, pair_sem, got_sem,
):
    my_s = lax.axis_index("seq")
    my_m = lax.axis_index("mp")
    total = n_seq * n_mp
    me = my_s * n_mp + my_m
    block = lat.shape[1] // parts
    piece = block // n_mp
    feats = lat.shape[2]
    tokens, width = bs_v.shape
    keys = k_v.shape[0]
    lanes = 2 * HEAD_DIM
    pairs = width // lanes
    rows = max(16, min(256, tokens, (256 * 512) // keys))
    blocks = tokens // rows
    tile = 256
    bf16, f32 = jnp.bfloat16, jnp.float32

    loads = [
        pltpu.make_async_copy(src, dst, load_sem.at[i])
        for i, (src, dst) in enumerate(
            [(bs, bs_v), (wq, wq_v), (wd, wd_v), (wk, wk_v), (wv, wv_v), (wo, wo_v)]
        )
    ]
    for load in loads:
        load.start()

    barrier = pltpu.get_barrier_semaphore()

    def greet(step, carry):
        other = lax.rem(me + step, total)
        pl.semaphore_signal(
            barrier, inc=1,
            device_id={"seq": other // n_mp, "mp": lax.rem(other, n_mp)},
            device_id_type=MESH,
        )
        return carry

    lax.fori_loop(1, total, greet, 0)
    pl.semaphore_wait(barrier, total - 1)

    def piece_of(h, t, m):
        return lat.at[t, pl.ds(pl.multiple_of(h * block + m * piece, piece), piece), :]

    def slot_of(h, s, m):
        return latbuf.at[h, m, pl.ds(pl.multiple_of(s * piece, piece), piece), :]

    def piece_copy(h, other):
        t, m = other // n_mp, lax.rem(other, n_mp)
        return pltpu.make_async_remote_copy(
            src_ref=piece_of(h, t, m),
            dst_ref=slot_of(h, my_s, my_m),
            send_sem=send_sem.at[h, other],
            recv_sem=recv_sem.at[h, me],
            device_id={"seq": t, "mp": m},
            device_id_type=MESH,
        )

    for h in range(parts):
        def send_piece(step, carry, h=h):
            piece_copy(h, lax.rem(me + step, total)).start()
            return carry

        lax.fori_loop(1, total, send_piece, 0)
        pltpu.make_async_copy(
            piece_of(h, my_s, my_m), slot_of(h, my_s, my_m), recv_sem.at[h, me]
        ).start()

    running = jnp.broadcast_to(lengths[...], (8, lengths.shape[1]))
    own_length = running
    lane_at = lax.broadcasted_iota(jnp.int32, running.shape, 1)
    shift = 1
    while shift < lengths.shape[1]:
        running = running + jnp.where(lane_at >= shift, pltpu.roll(running, shift, 1), 0)
        shift *= 2
    starts_v[...] = running - own_length
    v_ext[:, lanes:] = jnp.ones((keys, lanes), bf16)

    loads[0].wait()
    loads[1].wait()

    def query_tile(j, carry):
        cols = pl.ds(pl.multiple_of(j * tile, tile), tile)
        made = jnp.dot(bs_v[...], wq_v[:, cols], preferred_element_type=f32)
        q_v[:, cols] = made.astype(bf16) * bf16(HEAD_DIM**-0.5)
        return carry

    lax.fori_loop(0, width // tile, query_tile, 0)
    loads[2].wait()

    def project(h, first, last):
        def one(step, carry):
            m = lax.rem(my_m + step, n_mp)

            def arrived(s, inner_carry):
                here = slot_of(h, s, m)
                pltpu.make_async_copy(here, here, recv_sem.at[h, s * n_mp + m]).wait()
                return inner_carry

            lax.fori_loop(0, n_seq, arrived, 0)
            at = pl.ds(pl.multiple_of(m * feats, feats), feats)
            acc[...] += jnp.dot(latbuf[h, m], wd_v[at, :], preferred_element_type=f32)
            return carry

        if first == 0:
            acc[...] = jnp.zeros_like(acc)
        lax.fori_loop(first, last, one, 0)

    outer = n_mp // inner
    my_o = my_m // inner
    my_i = lax.rem(my_m, inner)
    partner = my_o * inner + (inner - 1 - my_i)
    has_up = my_o < outer - 1
    has_down = my_o > 0

    def row_copy(h, chunk, sem, target):
        return pltpu.make_async_remote_copy(
            src_ref=gbuf.at[h, :, chunk],
            dst_ref=gbuf.at[h, :, chunk],
            send_sem=sem.at[h, chunk],
            recv_sem=got_sem.at[h, chunk],
            device_id={"seq": my_s, "mp": target},
            device_id_type=MESH,
        )

    def wait_chunk(h, chunk):
        here = gbuf.at[h, :, chunk]
        pltpu.make_async_copy(here, here, got_sem.at[h, chunk]).wait()

    def go_up(h, chunk):
        return row_copy(h, chunk, up_sem, my_m + inner)

    def go_down(h, chunk):
        return row_copy(h, chunk, down_sem, my_m - inner)

    def go_pair(h, chunk):
        return row_copy(h, chunk, pair_sem, partner)

    def share(h):
        normed = rms_norm(acc[...], gain[...].astype(f32)[None, :]).astype(bf16)
        gbuf[h, :, my_m] = normed.reshape(n_seq, piece, width)
        pl.when(has_up)(lambda: go_up(h, my_m).start())
        pl.when(has_down)(lambda: go_down(h, my_m).start())
        go_pair(h, my_m).start()

    def relay(h, first, last):
        def one(k, carry):
            below = my_m - k * inner
            above = my_m + k * inner

            @pl.when(my_o - k >= 0)
            def _():
                wait_chunk(h, below)
                pl.when(has_up)(lambda: go_up(h, below).start())
                go_pair(h, below).start()

            @pl.when(my_o + k < outer)
            def _():
                wait_chunk(h, above)
                pl.when(has_down)(lambda: go_down(h, above).start())
                go_pair(h, above).start()

            return carry

        lax.fori_loop(first, last, one, 0)

    def take_pair(h):
        def one(o, carry):
            wait_chunk(h, o * inner + (inner - 1 - my_i))
            return carry

        lax.fori_loop(0, outer, one, 0)

    def keys_values(h):
        slab = min(keys, 512)

        def one(j, carry):
            cols = pl.ds(pl.multiple_of(j * tile, tile), tile)
            normed = gbuf[h].reshape(keys, width)
            for c in range(keys // slab):
                at = slice(c * slab, (c + 1) * slab)
                k_v[at, cols] = jnp.dot(
                    normed[at], wk_v[:, cols], preferred_element_type=f32
                ).astype(bf16)
                v_v[at, cols] = jnp.dot(
                    normed[at], wv_v[:, cols], preferred_element_type=f32
                ).astype(bf16)
            return carry

        lax.fori_loop(0, width // tile, one, 0)

    def mask(h):
        starts = jnp.concatenate(
            [
                starts_v[0:1, (s * parts + h) * block:(s * parts + h + 1) * block]
                for s in range(n_seq)
            ],
            axis=1,
        )
        position = my_m * tokens + lax.broadcasted_iota(jnp.int32, (tokens, 1), 0)
        bias[...] = jnp.where(starts <= position, 0.0, MASKED)

    low = lax.broadcasted_iota(jnp.int32, (rows, lanes), 1) < HEAD_DIM

    def attend(h, first, last):
        def one_pair(pair, carry):
            cols = pl.ds(pl.multiple_of(pair * lanes, lanes), lanes)
            v_ext[:, :lanes] = v_v[:, cols]

            def one_block(b, inner_carry):
                at = pl.ds(pl.multiple_of(b * rows, rows), rows)
                both = q_v[at, cols]
                made = []
                for half in range(2):
                    keep = low if half == 0 else ~low
                    q_half = jnp.where(keep, both, jnp.zeros_like(both))
                    scores = lax.dot_general(
                        q_half, k_v[:, cols], (((1,), (1,)), ((), ())),
                        preferred_element_type=f32,
                    ) + bias[at, :]
                    top = jnp.max(scores, axis=-1, keepdims=True)
                    weights = jnp.exp(scores - top).astype(bf16)
                    made.append(
                        (jnp.dot(weights, v_ext[...], preferred_element_type=f32), top)
                    )
                (sum0, top0), (sum1, top1) = made
                part = jnp.where(low, sum0[:, :lanes], sum1[:, :lanes])
                count = jnp.where(low, sum0[:, lanes:], sum1[:, lanes:])
                top = jnp.where(low, top0, top1)
                if h > 0:
                    before = peak[at, cols]
                    raised = jnp.maximum(before, top)
                    old, new = jnp.exp(before - raised), jnp.exp(top - raised)
                    part = num[at, cols] * old + part * new
                    count = den[at, cols] * old + count * new
                    top = raised
                if h == parts - 1:
                    head_out[at, cols] = (part / count).astype(bf16)
                else:
                    num[at, cols] = part
                    den[at, cols] = count
                    peak[at, cols] = top
                return inner_carry

            lax.fori_loop(0, blocks, one_block, 0, unroll=blocks <= 2)
            return carry

        lax.fori_loop(first, last, one_pair, 0)

    third = (outer + 1) // 3
    cut1, cut2 = min(1 + third, outer), min(1 + 2 * third, outer)
    project(0, 0, n_mp)
    share(0)
    relay(0, 1, cut1)
    project(1, 0, n_mp // 2)
    relay(0, cut1, cut2)
    project(1, n_mp // 2, n_mp)
    share(1)
    relay(0, cut2, outer)
    mask(0)
    loads[3].wait()
    loads[4].wait()
    loads[5].wait()
    relay(1, 1, cut1)
    take_pair(0)
    keys_values(0)
    relay(1, cut1, cut2)
    attend(0, 0, pairs // 2)
    relay(1, cut2, outer)
    attend(0, pairs // 2, pairs)
    mask(1)
    take_pair(1)
    keys_values(1)
    attend(1, 0, pairs)

    out_rows = min(tokens, 256)
    for r in range(tokens // out_rows):
        at = slice(r * out_rows, (r + 1) * out_rows)
        residual = bs_v[at, :].astype(f32) + jnp.dot(
            head_out[at, :], wo_v[...], preferred_element_type=f32
        )
        out[at, :] = rms_norm(residual, out_gain[...].astype(f32)[None, :]).astype(out.dtype)

    for h in range(parts):
        def finish_piece(step, carry, h=h):
            piece_copy(h, lax.rem(me + step, total)).wait_send()
            return carry

        lax.fori_loop(1, total, finish_piece, 0)

        def finish_rows(o, carry, h=h):
            chunk = o * inner + my_i
            pl.when(has_up & (o <= my_o))(lambda: go_up(h, chunk).wait_send())
            pl.when(has_down & (o >= my_o))(lambda: go_down(h, chunk).wait_send())
            go_pair(h, chunk).wait_send()
            return carry

        lax.fori_loop(0, outer, finish_rows, 0)


def per_device(n_seq, n_mp, byte_states, patch_latents, patch_lengths, w_down, kv_gain,
               w_query, w_key, w_value, w_out, out_gain):
    own_rows = byte_states[0]
    tokens, width = own_rows.shape
    patches = patch_lengths.shape[1]
    feats = patch_latents.shape[2]
    inner, parts = 2, 2
    here = patches // n_mp // parts
    keys = patches // parts
    any_spec = pl.BlockSpec(memory_space=pl.ANY)
    vmem_spec = pl.BlockSpec(memory_space=pltpu.VMEM)
    bf16, f32 = jnp.bfloat16, jnp.float32
    decoded = pl.pallas_call(
        functools.partial(layer_kernel, n_seq, n_mp, inner, parts),
        name="layer",
        out_shape=jax.ShapeDtypeStruct((tokens, width), bf16),
        in_specs=[any_spec, any_spec, vmem_spec] + [any_spec] * 5 + [vmem_spec] * 2,
        out_specs=vmem_spec,
        scratch_shapes=[
            pltpu.VMEM((parts, n_mp, here, feats), bf16),
            pltpu.VMEM((parts, n_seq, n_mp, here // n_seq, width), bf16),
            pltpu.VMEM((here, width), f32),
            pltpu.VMEM(w_down.shape, bf16),
            pltpu.VMEM((tokens, width), bf16),
            pltpu.VMEM(w_query.shape, bf16),
            pltpu.VMEM(w_key.shape, bf16),
            pltpu.VMEM(w_value.shape, bf16),
            pltpu.VMEM(w_out.shape, bf16),
            pltpu.VMEM((tokens, width), bf16),
            pltpu.VMEM((keys, width), bf16),
            pltpu.VMEM((keys, width), bf16),
            pltpu.VMEM((keys, 4 * HEAD_DIM), bf16),
            pltpu.VMEM((8, patches), jnp.int32),
            pltpu.VMEM((tokens, keys), f32),
            pltpu.VMEM((tokens, width), f32),
            pltpu.VMEM((tokens, width), f32),
            pltpu.VMEM((tokens, width), f32),
            pltpu.VMEM((tokens, width), bf16),
            pltpu.SemaphoreType.DMA((6,)),
            pltpu.SemaphoreType.DMA((parts, n_seq * n_mp)),
            pltpu.SemaphoreType.DMA((parts, n_seq * n_mp)),
            pltpu.SemaphoreType.DMA((parts, n_mp)),
            pltpu.SemaphoreType.DMA((parts, n_mp)),
            pltpu.SemaphoreType.DMA((parts, n_mp)),
            pltpu.SemaphoreType.DMA((parts, n_mp)),
        ],
        compiler_params=pltpu.CompilerParams(
            collective_id=0, has_side_effects=True, vmem_limit_bytes=63 * 1024 * 1024
        ),
    )(patch_latents, w_down, kv_gain, own_rows, w_query, w_key, w_value, w_out,
      out_gain, patch_lengths)
    return decoded[None]


def solution(mesh):
    return jax.shard_map(
        functools.partial(per_device, mesh.shape["seq"], mesh.shape["mp"]),
        mesh=mesh,
        in_specs=(
            P("seq", "mp", None),
            P(None, "seq", "mp"),
            P("seq", None),
            P(), P(), P(), P(), P(), P(), P(),
        ),
        out_specs=P("seq", "mp", None),
        check_vma=False,
    )
```

```python
import functools

import jax
import jax.numpy as jnp
from jax import lax
from jax.experimental import pallas as pl
from jax.experimental.pallas import tpu as pltpu
from jax.sharding import PartitionSpec as P

HEADS = 16
HEAD_DIM = 64
MASKED = -1e30
MESH = pl.DeviceIdType.MESH


def rms_norm(values, gain_row):
    mean_square = jnp.mean(values * values, axis=-1, keepdims=True)
    return values * lax.rsqrt(mean_square + 1e-05) * gain_row


def layer_kernel(
    n_seq, n_mp, inner, parts,
    lat, wd, gain, bs, wq, wk, wv, wo, lengths,
    out,
    latbuf, gbuf, acc, wd_v, bs_v, wq_v, wk_v, wv_v, wo_v,
    q_v, k_v, v_v, v_ext, starts_v, bias, num, den, peak, head_out,
    load_sem, send_sem, recv_sem, up_sem, down_sem, pair_sem, got_sem,
):
    my_s = lax.axis_index("seq")
    my_m = lax.axis_index("mp")
    total = n_seq * n_mp
    me = my_s * n_mp + my_m
    block = lat.shape[1] // parts
    piece = block // n_mp
    feats = lat.shape[2]
    tokens, width = bs_v.shape
    keys = k_v.shape[0]
    lanes = 2 * HEAD_DIM
    pairs = width // lanes
    rows = max(16, min(256, tokens, (256 * 512) // keys))
    blocks = tokens // rows
    tile = 256
    bf16, f32 = jnp.bfloat16, jnp.float32

    loads = [
        pltpu.make_async_copy(src, dst, load_sem.at[i])
        for i, (src, dst) in enumerate(
            [(bs, bs_v), (wq, wq_v), (wd, wd_v), (wk, wk_v), (wv, wv_v), (wo, wo_v)]
        )
    ]
    for load in loads:
        load.start()

    barrier = pltpu.get_barrier_semaphore()

    def greet(step, carry):
        other = lax.rem(me + step, total)
        pl.semaphore_signal(
            barrier, inc=1,
            device_id={"seq": other // n_mp, "mp": lax.rem(other, n_mp)},
            device_id_type=MESH,
        )
        return carry

    lax.fori_loop(1, total, greet, 0)
    pl.semaphore_wait(barrier, total - 1)

    def piece_of(h, t, m):
        return lat.at[t, pl.ds(pl.multiple_of(h * block + m * piece, piece), piece), :]

    def slot_of(h, s, m):
        return latbuf.at[h, m, pl.ds(pl.multiple_of(s * piece, piece), piece), :]

    def piece_copy(h, other):
        t, m = other // n_mp, lax.rem(other, n_mp)
        return pltpu.make_async_remote_copy(
            src_ref=piece_of(h, t, m),
            dst_ref=slot_of(h, my_s, my_m),
            send_sem=send_sem.at[h, other],
            recv_sem=recv_sem.at[h, me],
            device_id={"seq": t, "mp": m},
            device_id_type=MESH,
        )

    def send_pieces(h, first, last):
        def send_piece(step, carry):
            piece_copy(h, lax.rem(me + step, total)).start()
            return carry

        lax.fori_loop(first, last, send_piece, 0)

    for h in range(parts):
        send_pieces(h, 1, total)
    for h in range(parts):
        pltpu.make_async_copy(
            piece_of(h, my_s, my_m), slot_of(h, my_s, my_m), recv_sem.at[h, me]
        ).start()

    running = jnp.broadcast_to(lengths[...], (8, lengths.shape[1]))
    own_length = running
    lane_at = lax.broadcasted_iota(jnp.int32, running.shape, 1)
    shift = 1
    while shift < lengths.shape[1]:
        running = running + jnp.where(lane_at >= shift, pltpu.roll(running, shift, 1), 0)
        shift *= 2
    starts_v[...] = running - own_length
    v_ext[:, lanes:] = jnp.ones((keys, lanes), bf16)

    loads[0].wait()
    loads[1].wait()

    def query_tile(j, carry):
        cols = pl.ds(pl.multiple_of(j * tile, tile), tile)
        made = jnp.dot(bs_v[...], wq_v[:, cols], preferred_element_type=f32)
        q_v[:, cols] = made.astype(bf16) * bf16(HEAD_DIM**-0.5)
        return carry

    lax.fori_loop(0, width // tile, query_tile, 0)
    loads[2].wait()

    def project(h, first, last):
        def one(step, carry):
            m = lax.rem(my_m + step, n_mp)

            def arrived(s, inner_carry):
                here = slot_of(h, s, m)
                pltpu.make_async_copy(here, here, recv_sem.at[h, s * n_mp + m]).wait()
                return inner_carry

            lax.fori_loop(0, n_seq, arrived, 0)
            at = pl.ds(pl.multiple_of(m * feats, feats), feats)
            acc[...] += jnp.dot(latbuf[h, m], wd_v[at, :], preferred_element_type=f32)
            return carry

        if first == 0:
            acc[...] = jnp.zeros_like(acc)
        lax.fori_loop(first, last, one, 0)

    outer = n_mp // inner
    my_o = my_m // inner
    my_i = lax.rem(my_m, inner)
    partner = my_o * inner + (inner - 1 - my_i)
    has_up = my_o < outer - 1
    has_down = my_o > 0

    def row_copy(h, chunk, sem, target):
        return pltpu.make_async_remote_copy(
            src_ref=gbuf.at[h, :, chunk],
            dst_ref=gbuf.at[h, :, chunk],
            send_sem=sem.at[h, chunk],
            recv_sem=got_sem.at[h, chunk],
            device_id={"seq": my_s, "mp": target},
            device_id_type=MESH,
        )

    def wait_chunk(h, chunk):
        here = gbuf.at[h, :, chunk]
        pltpu.make_async_copy(here, here, got_sem.at[h, chunk]).wait()

    def go_up(h, chunk):
        return row_copy(h, chunk, up_sem, my_m + inner)

    def go_down(h, chunk):
        return row_copy(h, chunk, down_sem, my_m - inner)

    def go_pair(h, chunk):
        return row_copy(h, chunk, pair_sem, partner)

    def share(h):
        normed = rms_norm(acc[...], gain[...].astype(f32)[None, :]).astype(bf16)
        gbuf[h, :, my_m] = normed.reshape(n_seq, piece, width)
        pl.when(has_up)(lambda: go_up(h, my_m).start())
        pl.when(has_down)(lambda: go_down(h, my_m).start())
        go_pair(h, my_m).start()

    def relay(h, first, last):
        def one(k, carry):
            below = my_m - k * inner
            above = my_m + k * inner

            @pl.when(my_o - k >= 0)
            def _():
                wait_chunk(h, below)
                pl.when(has_up)(lambda: go_up(h, below).start())
                go_pair(h, below).start()

            @pl.when(my_o + k < outer)
            def _():
                wait_chunk(h, above)
                pl.when(has_down)(lambda: go_down(h, above).start())
                go_pair(h, above).start()

            return carry

        lax.fori_loop(first, last, one, 0)

    def take_pair(h):
        def one(o, carry):
            wait_chunk(h, o * inner + (inner - 1 - my_i))
            return carry

        lax.fori_loop(0, outer, one, 0)

    def keys_values(h):
        slab = min(keys, 512)

        def one(j, carry):
            cols = pl.ds(pl.multiple_of(j * tile, tile), tile)
            normed = gbuf[h].reshape(keys, width)
            for c in range(keys // slab):
                at = slice(c * slab, (c + 1) * slab)
                k_v[at, cols] = jnp.dot(
                    normed[at], wk_v[:, cols], preferred_element_type=f32
                ).astype(bf16)
                v_v[at, cols] = jnp.dot(
                    normed[at], wv_v[:, cols], preferred_element_type=f32
                ).astype(bf16)
            return carry

        lax.fori_loop(0, width // tile, one, 0)

    def mask(h):
        starts = jnp.concatenate(
            [
                starts_v[0:1, (s * parts + h) * block:(s * parts + h + 1) * block]
                for s in range(n_seq)
            ],
            axis=1,
        )
        position = my_m * tokens + lax.broadcasted_iota(jnp.int32, (tokens, 1), 0)
        bias[...] = jnp.where(starts <= position, 0.0, MASKED)

    low = lax.broadcasted_iota(jnp.int32, (rows, lanes), 1) < HEAD_DIM

    def attend(h, first, last):
        def one_pair(pair, carry):
            cols = pl.ds(pl.multiple_of(pair * lanes, lanes), lanes)
            v_ext[:, :lanes] = v_v[:, cols]

            def one_block(b, inner_carry):
                at = pl.ds(pl.multiple_of(b * rows, rows), rows)
                both = q_v[at, cols]
                made = []
                for half in range(2):
                    keep = low if half == 0 else ~low
                    q_half = jnp.where(keep, both, jnp.zeros_like(both))
                    scores = lax.dot_general(
                        q_half, k_v[:, cols], (((1,), (1,)), ((), ())),
                        preferred_element_type=f32,
                    ) + bias[at, :]
                    top = jnp.max(scores, axis=-1, keepdims=True)
                    weights = jnp.exp(scores - top).astype(bf16)
                    made.append(
                        (jnp.dot(weights, v_ext[...], preferred_element_type=f32), top)
                    )
                (sum0, top0), (sum1, top1) = made
                part = jnp.where(low, sum0[:, :lanes], sum1[:, :lanes])
                count = jnp.where(low, sum0[:, lanes:], sum1[:, lanes:])
                top = jnp.where(low, top0, top1)
                if h > 0:
                    before = peak[at, cols]
                    raised = jnp.maximum(before, top)
                    old, new = jnp.exp(before - raised), jnp.exp(top - raised)
                    part = num[at, cols] * old + part * new
                    count = den[at, cols] * old + count * new
                    top = raised
                if h == parts - 1:
                    head_out[at, cols] = (part / count).astype(bf16)
                else:
                    num[at, cols] = part
                    den[at, cols] = count
                    peak[at, cols] = top
                return inner_carry

            lax.fori_loop(0, blocks, one_block, 0, unroll=blocks <= 2)
            return carry

        lax.fori_loop(first, last, one_pair, 0)

    third = (outer + 1) // 3
    cut1, cut2 = min(1 + third, outer), min(1 + 2 * third, outer)
    project(0, 0, n_mp)
    share(0)
    relay(0, 1, cut1)
    project(1, 0, n_mp // 2)
    relay(0, cut1, cut2)
    project(1, n_mp // 2, n_mp)
    share(1)
    relay(0, cut2, outer)
    mask(0)
    loads[3].wait()
    loads[4].wait()
    loads[5].wait()
    relay(1, 1, cut1)
    take_pair(0)
    keys_values(0)
    relay(1, cut1, cut2)
    attend(0, 0, pairs // 2)
    relay(1, cut2, outer)
    attend(0, pairs // 2, pairs)
    mask(1)
    take_pair(1)
    keys_values(1)
    attend(1, 0, pairs)

    out_rows = min(tokens, 256)
    for r in range(tokens // out_rows):
        at = slice(r * out_rows, (r + 1) * out_rows)
        residual = bs_v[at, :].astype(f32) + jnp.dot(
            head_out[at, :], wo_v[...], preferred_element_type=f32
        )
        mean_square = jnp.mean(residual * residual, axis=-1, keepdims=True)
        out[at, :] = residual * lax.rsqrt(mean_square + 1e-05)

    for h in range(parts):
        def finish_piece(step, carry, h=h):
            piece_copy(h, lax.rem(me + step, total)).wait_send()
            return carry

        lax.fori_loop(1, total, finish_piece, 0)

        def finish_rows(o, carry, h=h):
            chunk = o * inner + my_i
            pl.when(has_up & (o <= my_o))(lambda: go_up(h, chunk).wait_send())
            pl.when(has_down & (o >= my_o))(lambda: go_down(h, chunk).wait_send())
            go_pair(h, chunk).wait_send()
            return carry

        lax.fori_loop(0, outer, finish_rows, 0)


def per_device(n_seq, n_mp, byte_states, patch_latents, patch_lengths, w_down, kv_gain,
               w_query, w_key, w_value, w_out, out_gain):
    own_rows = byte_states[0]
    tokens, width = own_rows.shape
    patches = patch_lengths.shape[1]
    feats = patch_latents.shape[2]
    inner, parts = 2, 2
    here = patches // n_mp // parts
    keys = patches // parts
    any_spec = pl.BlockSpec(memory_space=pl.ANY)
    vmem_spec = pl.BlockSpec(memory_space=pltpu.VMEM)
    bf16, f32 = jnp.bfloat16, jnp.float32
    decoded = pl.pallas_call(
        functools.partial(layer_kernel, n_seq, n_mp, inner, parts),
        name="layer",
        out_shape=jax.ShapeDtypeStruct((tokens, width), f32),
        in_specs=[any_spec, any_spec, vmem_spec] + [any_spec] * 5 + [vmem_spec],
        out_specs=vmem_spec,
        scratch_shapes=[
            pltpu.VMEM((parts, n_mp, here, feats), bf16),
            pltpu.VMEM((parts, n_seq, n_mp, here // n_seq, width), bf16),
            pltpu.VMEM((here, width), f32),
            pltpu.VMEM(w_down.shape, bf16),
            pltpu.VMEM((tokens, width), bf16),
            pltpu.VMEM(w_query.shape, bf16),
            pltpu.VMEM(w_key.shape, bf16),
            pltpu.VMEM(w_value.shape, bf16),
            pltpu.VMEM(w_out.shape, bf16),
            pltpu.VMEM((tokens, width), bf16),
            pltpu.VMEM((keys, width), bf16),
            pltpu.VMEM((keys, width), bf16),
            pltpu.VMEM((keys, 4 * HEAD_DIM), bf16),
            pltpu.VMEM((8, patches), jnp.int32),
            pltpu.VMEM((tokens, keys), f32),
            pltpu.VMEM((tokens, width), f32),
            pltpu.VMEM((tokens, width), f32),
            pltpu.VMEM((tokens, width), f32),
            pltpu.VMEM((tokens, width), bf16),
            pltpu.SemaphoreType.DMA((6,)),
            pltpu.SemaphoreType.DMA((parts, n_seq * n_mp)),
            pltpu.SemaphoreType.DMA((parts, n_seq * n_mp)),
            pltpu.SemaphoreType.DMA((parts, n_mp)),
            pltpu.SemaphoreType.DMA((parts, n_mp)),
            pltpu.SemaphoreType.DMA((parts, n_mp)),
            pltpu.SemaphoreType.DMA((parts, n_mp)),
        ],
        compiler_params=pltpu.CompilerParams(
            collective_id=0, has_side_effects=True, vmem_limit_bytes=63 * 1024 * 1024
        ),
    )(patch_latents, w_down, kv_gain, own_rows, w_query, w_key, w_value, w_out,
      patch_lengths)
    return (decoded * out_gain.astype(f32)).astype(bf16)[None]


def solution(mesh):
    return jax.shard_map(
        functools.partial(per_device, mesh.shape["seq"], mesh.shape["mp"]),
        mesh=mesh,
        in_specs=(
            P("seq", "mp", None),
            P(None, "seq", "mp"),
            P("seq", None),
            P(), P(), P(), P(), P(), P(), P(),
        ),
        out_specs=P("seq", "mp", None),
        check_vma=False,
    )
```
